32 devices in a mesh: shard: 16 (over z, y, core), model: 2 (over x).
Axes of the slice: x: 2, y: 2, z: 4, core: 2. Of those that a mesh axis runs over, the one named last changes fastest.
Arguments:
- gradients: float32 [128, 128, 4096], P(None, 'shard', 'model'), may hold values from -6 to 6
- momentum: float32 [128, 128, 4096], P(None, 'shard', 'model'), may hold values from -6 to 6
- weights: float32 [128, 128, 4096], P(None, 'shard', 'model'), may hold values from -0.1875 to 0.1875
Outputs:
- new_weights: float32 [128, 128, 4096], P(None, 'shard', 'model')
- new_momentum: float32 [128, 128, 4096], P(None, 'shard', 'model')
The draws below stay inside these ranges and needn't reach their ends.
All inputs are finite; a program needn't handle non-finite values.
Results may differ from the reference program's by a relative error of at most 0.0001.
Values sent between devices are 32-bit elements; how exact they have to be, the bound alone decides.
No kernel may reach another device: no remote copies, remote signals or barrier semaphores. Data moves between devices by JAX's collectives and lax.ppermute only.
A program may use at most 128 MiB of HBM per device.

```python
import jax
import jax.numpy as jnp
from jax import lax

SIDE = 128
WIDE = 4096
MATS = 128
ITERS = 3


def steps_of(stream_key, shape, pieces, low, largest):
    loudness, own = 1.0, jax.random.fold_in(stream_key, 6)
    for dim, parts in pieces:
        steps = jnp.exp(jax.random.uniform(jax.random.fold_in(own, dim), (parts,), jnp.float32, low / len(pieces), largest / len(pieces)))
        loudness = loudness * jnp.repeat(steps, shape[dim] // parts).reshape([-1 if axis == dim else 1 for axis in range(len(shape))])
    return loudness


def scatter_about(rng, shape, spread, bound, split=(), kind=jnp.bfloat16):
    entries = spread * jax.random.normal(rng, shape, jnp.float32)
    if split:
        entries = entries * steps_of(rng, shape, split, -0.22, 0.18)
    return jnp.clip(entries, -bound, bound).astype(kind)


def setup_inputs(seed: int = 0) -> dict:
    key_of = jax.random.split(jax.random.key(seed), 4)
    gradients = scatter_about(key_of[0], (MATS, SIDE, WIDE), 1.0, 6.0, ((1, 16), (2, 2)), jnp.float32)
    momentum = scatter_about(key_of[1], (MATS, SIDE, WIDE), 1.0, 6.0, ((1, 16), (2, 2)), jnp.float32)
    weights = scatter_about(key_of[2], (MATS, SIDE, WIDE), 0.03, 0.1875, ((1, 16), (2, 2)), jnp.float32)
    return dict(gradients=gradients, momentum=momentum, weights=weights)


hold_rate = 0.9
learn_rate = 0.9
decay_rate = 0.1

def reference(gradients, momentum, weights):
    new_momentum = hold_rate * momentum + gradients

    def orthogonal_one(stack):
        iterate = stack[None]
        iterate = iterate * lax.rsqrt(lax.optimization_barrier(jnp.sum(iterate * iterate, axis=(1, 2), keepdims=True)) + 1e-06)
        for step in range(ITERS):
            gram = jnp.einsum('mik,mjk->mij', iterate, iterate, precision=lax.Precision.HIGHEST)
            mixed = -4.775 * gram + 2.0315 * jnp.einsum('mij,mjk->mik', gram, gram, precision=lax.Precision.HIGHEST)
            iterate = 3.4445 * iterate + jnp.einsum('mij,mjk->mik', mixed, iterate, precision=lax.Precision.HIGHEST)
        return iterate[0]
    iterate = lax.map(orthogonal_one, new_momentum)
    new_weights = (1.0 - learn_rate * decay_rate) * weights - learn_rate * iterate
    return (new_weights, new_momentum)
```

```python
import functools

import jax
import jax.numpy as jnp
from jax import lax
from jax.experimental import pallas as pl
from jax.experimental.pallas import tpu as pltpu
from jax.sharding import PartitionSpec as P

ITERS = 3
CHUNKS = 4

hold_rate = 0.9
learn_rate = 0.9
decay_rate = 0.1


def mm(form, a, b):
    return jnp.einsum(form, a, b, precision=lax.Precision.HIGHEST)


def dot(a, b, contract_b=0):
    return lax.dot_general(
        a, b, (((1,), (contract_b,)), ((), ())),
        precision=lax.Precision.HIGHEST, preferred_element_type=jnp.float32,
    )


def cost(flops, moved):
    return pl.CostEstimate(flops=flops, bytes_accessed=moved, transcendentals=0)


def over_model(part):
    size = lax.axis_size("model")
    total = part
    for hop in range(1, size):
        total = total + lax.ppermute(part, "model", [(i, (i + hop) % size) for i in range(size)])
    return total


def polynomial(raw, product):
    side = raw.shape[-1]
    place = raw.shape[:-2] + (side, side)
    eye = (lax.broadcasted_iota(jnp.int32, place, raw.ndim - 2) == lax.broadcasted_iota(jnp.int32, place, raw.ndim - 1)).astype(jnp.float32)
    total = jnp.sum(jnp.sum(raw * eye, axis=-1, keepdims=True), axis=-2, keepdims=True)
    scale = lax.rsqrt(total + 1e-06)
    gram = (raw * scale) * scale
    chain = None
    for step in range(ITERS):
        poly = 3.4445 * eye - 4.775 * gram + 2.0315 * product(gram, gram)
        chain = poly if chain is None else product(poly, chain)
        if step < ITERS - 1:
            gram = product(poly, product(gram, poly))
    return chain * scale


def momentum_kernel(gradients_ref, momentum_ref, *refs):
    whole_ref, piece_ref = refs[-2:]
    fresh = hold_rate * momentum_ref[...] + gradients_ref[...]
    whole_ref[...] = fresh
    piece_ref[...] = fresh


def momentum_chunk(chunk, gradients, momentum, whole):
    mats, rows, columns = gradients.shape
    count = mats // CHUNKS
    block = min(count, 8)
    first = chunk * count // block
    there = pl.BlockSpec((block, rows, columns), lambda i: (i + first, 0, 0))
    here = pl.BlockSpec((block, rows, columns), lambda i: (i, 0, 0))
    size = count * rows * columns
    return pl.pallas_call(
        momentum_kernel,
        grid=(count // block,),
        in_specs=[there, there] + ([] if whole is None else [pl.BlockSpec(memory_space=pl.ANY)]),
        out_specs=[there, here],
        out_shape=[jax.ShapeDtypeStruct(gradients.shape, jnp.float32), jax.ShapeDtypeStruct((count, rows, columns), jnp.float32)],
        input_output_aliases={} if whole is None else {2: 0},
        cost_estimate=cost(2 * size, 16 * size),
        name="momentum",
    )(gradients, momentum, *([] if whole is None else [whole]))


def weights_kernel(weights_ref, back_ref, *refs):
    refs[-1][...] = (1.0 - learn_rate * decay_rate) * weights_ref[...] - learn_rate * back_ref[...]


def weights_chunk(chunk, weights, back, whole):
    mats, rows, columns = weights.shape
    count = mats // CHUNKS
    block = min(count, 8)
    first = chunk * count // block
    there = pl.BlockSpec((block, rows, columns), lambda i: (i + first, 0, 0))
    here = pl.BlockSpec((block, rows, columns), lambda i: (i, 0, 0))
    size = count * rows * columns
    return pl.pallas_call(
        weights_kernel,
        grid=(count // block,),
        in_specs=[there, here] + ([] if whole is None else [pl.BlockSpec(memory_space=pl.ANY)]),
        out_specs=there,
        out_shape=jax.ShapeDtypeStruct(weights.shape, jnp.float32),
        input_output_aliases={} if whole is None else {2: 0},
        cost_estimate=cost(3 * size, 12 * size),
        name="weights",
    )(weights, back, *([] if whole is None else [whole]))


def gram_kernel(stack_ref, out_ref):
    owners, _, rows, columns = stack_ref.shape
    stack = stack_ref[...].reshape(owners * rows, columns)
    out_ref[0] = dot(stack, stack, 1)


def gram_of(arrived):
    owners, mats, rows, columns = arrived.shape
    side = owners * rows
    return pl.pallas_call(
        gram_kernel,
        grid=(mats,),
        in_specs=[pl.BlockSpec((owners, 1, rows, columns), lambda i: (0, i, 0, 0))],
        out_specs=pl.BlockSpec((1, side, side), lambda i: (i, 0, 0)),
        out_shape=jax.ShapeDtypeStruct((mats, side, side), jnp.float32),
        cost_estimate=cost(12 * mats * side * side * columns, 4 * mats * side * columns),
        name="gram",
    )(arrived)


def apply_kernel(gram_ref, stack_ref, out_ref):
    owners, _, rows, columns = stack_ref.shape
    chain = polynomial(gram_ref[0], dot)
    stack = stack_ref[...].reshape(owners * rows, columns)
    out_ref[...] = dot(chain, stack).reshape(owners, 1, rows, columns)


def apply_of(gram, arrived):
    owners, mats, rows, columns = arrived.shape
    side = owners * rows
    spot = pl.BlockSpec((owners, 1, rows, columns), lambda i: (0, i, 0, 0))
    return pl.pallas_call(
        apply_kernel,
        grid=(mats,),
        in_specs=[pl.BlockSpec((1, side, side), lambda i: (i, 0, 0)), spot],
        out_specs=spot,
        out_shape=jax.ShapeDtypeStruct(arrived.shape, jnp.float32),
        cost_estimate=cost(12 * mats * side * side * (columns + 9 * side), 8 * mats * side * columns),
        name="apply",
    )(gram, arrived)


def exchange(piece):
    return lax.all_to_all(piece, "shard", split_axis=0, concat_axis=0, tiled=True)


def body(gradients, momentum, weights):
    owners = lax.axis_size("shard")
    mats, rows, columns = gradients.shape
    held = mats // (CHUNKS * owners)
    whole, arrived = None, []
    for c in range(CHUNKS):
        whole, piece = momentum_chunk(c, gradients, momentum, whole)
        arrived.append(exchange(piece.reshape(owners, held, rows, columns)))
    updated = None
    for c in range(CHUNKS):
        gram = over_model(gram_of(arrived[c]))
        back = exchange(apply_of(gram, arrived[c]))
        updated = weights_chunk(c, weights, back.reshape(owners * held, rows, columns), updated)
    return (updated, whole)


def small_body(gradients, momentum, weights):
    new_momentum = hold_rate * momentum + gradients
    stack = lax.all_to_all(new_momentum, "shard", split_axis=0, concat_axis=1, tiled=True)
    gram = over_model(mm("mik,mjk->mij", stack, stack))
    chain = polynomial(gram, functools.partial(mm, "mij,mjk->mik"))
    back = lax.all_to_all(mm("mij,mjk->mik", chain, stack), "shard", split_axis=1, concat_axis=0, tiled=True)
    return ((1.0 - learn_rate * decay_rate) * weights - learn_rate * back, new_momentum)


def pick(gradients, momentum, weights):
    mats, rows, columns = gradients.shape
    fits = rows % 8 == 0 and columns % 128 == 0 and mats % (CHUNKS * lax.axis_size("shard")) == 0
    return (body if fits else small_body)(gradients, momentum, weights)


def solution(mesh):
    placed = P(None, "shard", "model")
    return jax.shard_map(pick, mesh=mesh, in_specs=(placed,) * 3, out_specs=(placed,) * 2, check_vma=False)
```

```python
import functools

import jax
import jax.numpy as jnp
from jax import lax
from jax.experimental import pallas as pl
from jax.experimental.pallas import tpu as pltpu
from jax.sharding import PartitionSpec as P


ITERS = 3
CHUNKS = 2
FAR = 4
NEAR = 3
HEAD = (2, 6)
TAIL = 3
LAST = (8, 4)

hold_rate = 0.9
learn_rate = 0.9
decay_rate = 0.1


def mm(form, a, b):
    return jnp.einsum(form, a, b, precision=lax.Precision.HIGHEST)


def dot(a, b, contract_b=0):
    return lax.dot_general(
        a, b, (((1,), (contract_b,)), ((), ())),
        precision=lax.Precision.HIGHEST, preferred_element_type=jnp.float32,
    )


def cost(flops, moved):
    return pl.CostEstimate(flops=flops, bytes_accessed=moved, transcendentals=0)


def around(part, axis):
    size = lax.axis_size(axis)
    return [lax.ppermute(part, axis, [(i, (i + hop) % size) for i in range(size)]) for hop in range(1, size)]


def polynomial(raw, product):
    side = raw.shape[-1]
    place = raw.shape[:-2] + (side, side)
    eye = (lax.broadcasted_iota(jnp.int32, place, raw.ndim - 2) == lax.broadcasted_iota(jnp.int32, place, raw.ndim - 1)).astype(jnp.float32)
    total = jnp.sum(jnp.sum(raw * eye, axis=-1, keepdims=True), axis=-2, keepdims=True)
    scale = lax.rsqrt(total + 1e-06)
    gram = (raw * scale) * scale
    chain = None
    for step in range(ITERS):
        poly = 3.4445 * eye - 4.775 * gram + 2.0315 * product(gram, gram)
        chain = poly if chain is None else product(poly, chain)
        if step < ITERS - 1:
            gram = product(poly, product(gram, poly))
    return chain * scale


def places(flips, held, rows, columns, chunk):
    def spot(i, me):
        flip = flips[0]
        for k in range(1, len(flips)):
            flip = jnp.where(i == k, flips[k], flip)
        return ((me[0] ^ flip) * CHUNKS + chunk, 0, 0)

    return pl.BlockSpec((held, rows, columns), spot)


def momentum_kernel(count, me_ref, gradients_ref, momentum_ref, *refs):
    whole_ref, piece_refs = refs[-count - 1], refs[-count:]
    fresh = hold_rate * momentum_ref[...] + gradients_ref[...]
    whole_ref[...] = fresh
    for k in range(count):
        @pl.when(pl.program_id(0) == k)
        def _():
            piece_refs[k][...] = fresh


def momentum_of(me, flips, chunk, held, gradients, momentum, whole):
    mats, rows, columns = gradients.shape
    count = len(flips)
    there = places(flips, held, rows, columns, chunk)
    here = pl.BlockSpec((held, rows, columns), lambda i, me: (0, 0, 0))
    size = count * held * rows * columns
    more = [] if whole is None else [whole]
    return pl.pallas_call(
        functools.partial(momentum_kernel, count),
        grid_spec=pltpu.PrefetchScalarGridSpec(
            num_scalar_prefetch=1,
            grid=(count,),
            in_specs=[there, there] + [pl.BlockSpec(memory_space=pl.ANY)] * len(more),
            out_specs=[there] + [here] * count,
        ),
        out_shape=[jax.ShapeDtypeStruct(gradients.shape, jnp.float32)]
        + [jax.ShapeDtypeStruct((held, rows, columns), jnp.float32)] * count,
        input_output_aliases={3: 0} if more else {},
        cost_estimate=cost(2 * size, 16 * size),
        name="momentum",
    )(me, gradients, momentum, *more)


def weights_kernel(count, me_ref, weights_ref, *refs):
    for k in range(count):
        @pl.when(pl.program_id(0) == k)
        def _():
            refs[-1][...] = (1.0 - learn_rate * decay_rate) * weights_ref[...] - learn_rate * refs[k][...]


def weights_of(me, flips, chunk, weights, back, whole):
    mats, rows, columns = weights.shape
    count, held = len(flips), back[0].shape[0]
    there = places(flips, held, rows, columns, chunk)
    here = pl.BlockSpec((held, rows, columns), lambda i, me: (0, 0, 0))
    size = count * held * rows * columns
    more = [] if whole is None else [whole]
    return pl.pallas_call(
        functools.partial(weights_kernel, count),
        grid_spec=pltpu.PrefetchScalarGridSpec(
            num_scalar_prefetch=1,
            grid=(count,),
            in_specs=[there] + [here] * count + [pl.BlockSpec(memory_space=pl.ANY)] * len(more),
            out_specs=there,
        ),
        out_shape=jax.ShapeDtypeStruct(weights.shape, jnp.float32),
        input_output_aliases={2 + count: 0} if more else {},
        cost_estimate=cost(3 * size, 12 * size),
        name="weights",
    )(me, weights, *back, *more)


def stacked(refs):
    return jnp.concatenate([ref[0] for ref in refs], axis=0)


def gram_kernel(*refs):
    stack = stacked(refs[:-1])
    refs[-1][0] = dot(stack, stack, 1)


def gram_of(pieces):
    held, rows, columns = pieces[0].shape
    side = len(pieces) * rows
    return pl.pallas_call(
        gram_kernel,
        grid=(held,),
        in_specs=[pl.BlockSpec((1, rows, columns), lambda i: (i, 0, 0))] * len(pieces),
        out_specs=pl.BlockSpec((1, side, side), lambda i: (i, 0, 0)),
        out_shape=jax.ShapeDtypeStruct((held, side, side), jnp.float32),
        cost_estimate=cost(12 * held * side * side * columns, 4 * held * side * columns),
        name="gram",
    )(*pieces)


def apply_kernel(parts, count, *refs):
    raw = refs[0][0]
    for ref in refs[1:parts]:
        raw = raw + ref[0]
    found = dot(polynomial(raw, dot), stacked(refs[parts:parts + count]))
    rows = found.shape[0] // count
    for k in range(count):
        refs[parts + count + k][0] = found[k * rows:(k + 1) * rows]


def apply_of(grams, pieces):
    held, rows, columns = pieces[0].shape
    side = len(pieces) * rows
    square = pl.BlockSpec((1, side, side), lambda i: (i, 0, 0))
    strip = pl.BlockSpec((1, rows, columns), lambda i: (i, 0, 0))
    return pl.pallas_call(
        functools.partial(apply_kernel, len(grams), len(pieces)),
        grid=(held,),
        in_specs=[square] * len(grams) + [strip] * len(pieces),
        out_specs=[strip] * len(pieces),
        out_shape=[jax.ShapeDtypeStruct((held, rows, columns), jnp.float32)] * len(pieces),
        cost_estimate=cost(12 * held * side * side * (columns + 9 * side), 8 * held * side * columns),
        name="apply",
    )(*grams, *pieces)


class Stream:
    def __init__(self):
        self.ends, self.gates = {True: [], False: []}, []

    def send(self, piece, flip):
        size = lax.axis_size("shard")
        far = flip >= size // 2
        ends, window = self.ends[far], FAR if far else NEAR
        gates = self.gates + ends[-window:][:len(ends) // window]
        if gates:
            piece = lax.optimization_barrier((piece, *gates[:len(self.gates) + 1]))[0]
        self.gates = []
        ends.append(lax.ppermute(piece, "shard", [(i, i ^ flip) for i in range(size)]))
        return ends[-1]


def woven(far, near):
    flips = []
    for k in range(max(len(far), len(near))):
        flips += far[k:k + 1] + near[k:k + 1]
    return flips


def parts(flips, sizes):
    for size in sizes:
        yield flips[:size]
        flips = flips[size:]
    if flips:
        yield flips


def body(gradients, momentum, weights):
    owners = lax.axis_size("shard")
    mats, rows, columns = gradients.shape
    held = mats // (CHUNKS * owners)
    far, near = list(range(owners // 2, owners)), list(range(1, owners // 2))
    flips = woven(far, near)
    me = lax.axis_index("shard").astype(jnp.int32).reshape(1)

    stream = Stream()
    whole, updated, arrived, grams, found, back = None, None, {}, {}, {}, {}

    def early(c):
        grams[c] = [gram_of([arrived[c][flip] for flip in range(owners)])]
        stream.gates.append(grams[c][0])

    def middle(c):
        grams[c] += around(grams[c][0], "model")

    def late(c):
        found[c] = apply_of(grams[c], [arrived[c][flip] for flip in range(owners)])
        stream.gates.append(found[c][0])

    def solve(c, flip):
        if flip == far[FAR]:
            early(c)
        if flip == far[FAR + 1]:
            middle(c)
            return
        if flip == far[FAR + 2]:
            late(c)

    for c in range(CHUNKS):
        arrived[c] = {}
        for some in parts(flips + [0], HEAD if c == 0 else ()):
            whole, *pieces = momentum_of(me, some, c, held, gradients, momentum, whole)
            for flip, piece in zip(some, pieces):
                if c > 0 and flip:
                    solve(c - 1, flip)
                arrived[c][flip] = stream.send(piece, flip) if flip else piece
    for c in range(CHUNKS):
        back[c] = {0: found[c][0]}
        for flip in flips if c < CHUNKS - 1 else woven(far[:-TAIL], near) + far[-TAIL:]:
            if c == 0:
                solve(CHUNKS - 1, flip)
            elif flip == far[FAR]:
                updated = weights_of(me, [0] + flips, c - 1, weights, [back[c - 1][k] for k in [0] + flips], updated)
                stream.gates.append(updated)
            back[c][flip] = stream.send(found[c][flip], flip)
    last = [0] + list(back[CHUNKS - 1])[1:]
    for some in parts(last, LAST):
        updated = weights_of(me, some, CHUNKS - 1, weights, [back[CHUNKS - 1][k] for k in some], updated)
    return (updated, whole)


def small_body(gradients, momentum, weights):
    new_momentum = hold_rate * momentum + gradients
    stack = lax.all_to_all(new_momentum, "shard", split_axis=0, concat_axis=1, tiled=True)
    gram = mm("mik,mjk->mij", stack, stack)
    gram = gram + sum(around(gram, "model"))
    chain = polynomial(gram, functools.partial(mm, "mij,mjk->mik"))
    back = lax.all_to_all(mm("mij,mjk->mik", chain, stack), "shard", split_axis=1, concat_axis=0, tiled=True)
    return ((1.0 - learn_rate * decay_rate) * weights - learn_rate * back, new_momentum)


def pick(gradients, momentum, weights):
    owners = lax.axis_size("shard")
    mats, rows, columns = gradients.shape
    fits = rows % 8 == 0 and columns % 128 == 0 and mats % (CHUNKS * owners) == 0 and owners & (owners - 1) == 0 and owners // 2 > FAR + 2
    return (body if fits else small_body)(gradients, momentum, weights)


def solution(mesh):
    placed = P(None, "shard", "model")
    return jax.shard_map(pick, mesh=mesh, in_specs=(placed,) * 3, out_specs=(placed,) * 2, check_vma=False)
```

```python
import functools

import jax
import jax.numpy as jnp
from jax import lax
from jax.experimental import pallas as pl
from jax.experimental.pallas import tpu as pltpu
from jax.sharding import PartitionSpec as P


ITERS = 3
CHUNKS = 2
FAR = 6
NEAR = 6
LATER = 1
HEAD = (2, 6)
TAIL = 3
LAST = (8, 4)

hold_rate = 0.9
learn_rate = 0.9
decay_rate = 0.1


def mm(form, a, b):
    return jnp.einsum(form, a, b, precision=lax.Precision.HIGHEST)


def dot(a, b, contract_b=0):
    return lax.dot_general(
        a, b, (((1,), (contract_b,)), ((), ())),
        precision=lax.Precision.HIGHEST, preferred_element_type=jnp.float32,
    )


def cost(flops, moved):
    return pl.CostEstimate(flops=flops, bytes_accessed=moved, transcendentals=0)


def around(part, axis):
    size = lax.axis_size(axis)
    return [lax.ppermute(part, axis, [(i, (i + hop) % size) for i in range(size)]) for hop in range(1, size)]


def polynomial(raw, product):
    side = raw.shape[-1]
    place = raw.shape[:-2] + (side, side)
    eye = (lax.broadcasted_iota(jnp.int32, place, raw.ndim - 2) == lax.broadcasted_iota(jnp.int32, place, raw.ndim - 1)).astype(jnp.float32)
    total = jnp.sum(jnp.sum(raw * eye, axis=-1, keepdims=True), axis=-2, keepdims=True)
    scale = lax.rsqrt(total + 1e-06)
    gram = (raw * scale) * scale
    chain = None
    for step in range(ITERS):
        poly = 3.4445 * eye - 4.775 * gram + 2.0315 * product(gram, gram)
        chain = poly if chain is None else product(poly, chain)
        if step < ITERS - 1:
            gram = product(poly, product(gram, poly))
    return chain * scale


def places(flips, held, rows, columns, chunk):
    def spot(i, me):
        flip = flips[0]
        for k in range(1, len(flips)):
            flip = jnp.where(i == k, flips[k], flip)
        return ((me[0] ^ flip) * CHUNKS + chunk, 0, 0)

    return pl.BlockSpec((held, rows, columns), spot)


def momentum_kernel(count, me_ref, gradients_ref, momentum_ref, *refs):
    whole_ref, piece_refs = refs[-count - 1], refs[-count:]
    fresh = hold_rate * momentum_ref[...] + gradients_ref[...]
    whole_ref[...] = fresh
    for k in range(count):
        @pl.when(pl.program_id(0) == k)
        def _():
            piece_refs[k][...] = fresh


def momentum_of(me, flips, chunk, held, gradients, momentum, whole):
    _, rows, columns = gradients.shape
    count = len(flips)
    there = places(flips, held, rows, columns, chunk)
    here = pl.BlockSpec((held, rows, columns), lambda i, me: (0, 0, 0))
    size = count * held * rows * columns
    more = [] if whole is None else [whole]
    return pl.pallas_call(
        functools.partial(momentum_kernel, count),
        grid_spec=pltpu.PrefetchScalarGridSpec(
            num_scalar_prefetch=1,
            grid=(count,),
            in_specs=[there, there] + [pl.BlockSpec(memory_space=pl.ANY)] * len(more),
            out_specs=[there] + [here] * count,
        ),
        out_shape=[jax.ShapeDtypeStruct(gradients.shape, jnp.float32)]
        + [jax.ShapeDtypeStruct((held, rows, columns), jnp.float32)] * count,
        input_output_aliases={3: 0} if more else {},
        cost_estimate=cost(2 * size, 16 * size),
        name="momentum",
    )(me, gradients, momentum, *more)


def weights_kernel(count, me_ref, weights_ref, *refs):
    for k in range(count):
        @pl.when(pl.program_id(0) == k)
        def _():
            refs[-1][...] = (1.0 - learn_rate * decay_rate) * weights_ref[...] - learn_rate * refs[k][...]


def weights_of(me, flips, chunk, weights, back, whole):
    _, rows, columns = weights.shape
    count, held = len(flips), back[0].shape[0]
    there = places(flips, held, rows, columns, chunk)
    here = pl.BlockSpec((held, rows, columns), lambda i, me: (0, 0, 0))
    size = count * held * rows * columns
    more = [] if whole is None else [whole]
    return pl.pallas_call(
        functools.partial(weights_kernel, count),
        grid_spec=pltpu.PrefetchScalarGridSpec(
            num_scalar_prefetch=1,
            grid=(count,),
            in_specs=[there] + [here] * count + [pl.BlockSpec(memory_space=pl.ANY)] * len(more),
            out_specs=there,
        ),
        out_shape=jax.ShapeDtypeStruct(weights.shape, jnp.float32),
        input_output_aliases={2 + count: 0} if more else {},
        cost_estimate=cost(3 * size, 12 * size),
        name="weights",
    )(me, weights, *back, *more)


def stacked(refs):
    return jnp.concatenate([ref[0] for ref in refs], axis=0)


def gram_kernel(*refs):
    stack = stacked(refs[:-1])
    refs[-1][0] = dot(stack, stack, 1)


def gram_of(pieces):
    held, rows, columns = pieces[0].shape
    side = len(pieces) * rows
    return pl.pallas_call(
        gram_kernel,
        grid=(held,),
        in_specs=[pl.BlockSpec((1, rows, columns), lambda i: (i, 0, 0))] * len(pieces),
        out_specs=pl.BlockSpec((1, side, side), lambda i: (i, 0, 0)),
        out_shape=jax.ShapeDtypeStruct((held, side, side), jnp.float32),
        cost_estimate=cost(12 * held * side * side * columns, 4 * held * side * columns),
        name="gram",
    )(*pieces)


def apply_kernel(parts, count, *refs):
    raw = refs[0][0]
    for ref in refs[1:parts]:
        raw = raw + ref[0]
    found = dot(polynomial(raw, dot), stacked(refs[parts:parts + count]))
    rows = found.shape[0] // count
    for k in range(count):
        refs[parts + count + k][0] = found[k * rows:(k + 1) * rows]


def apply_of(grams, pieces):
    held, rows, columns = pieces[0].shape
    side = len(pieces) * rows
    square = pl.BlockSpec((1, side, side), lambda i: (i, 0, 0))
    strip = pl.BlockSpec((1, rows, columns), lambda i: (i, 0, 0))
    return pl.pallas_call(
        functools.partial(apply_kernel, len(grams), len(pieces)),
        grid=(held,),
        in_specs=[square] * len(grams) + [strip] * len(pieces),
        out_specs=[strip] * len(pieces),
        out_shape=[jax.ShapeDtypeStruct((held, rows, columns), jnp.float32)] * len(pieces),
        cost_estimate=cost(12 * held * side * side * (columns + 9 * side), 8 * held * side * columns),
        name="apply",
    )(*grams, *pieces)


def woven(far, near):
    flips = []
    for k in range(max(len(far), len(near))):
        flips += far[k:k + 1] + near[k:k + 1]
    return flips


def cut(flips, sizes):
    runs = []
    for size in sizes:
        runs.append(tuple(flips[:size]))
        flips = flips[size:]
    return runs + [tuple(flips)] * bool(flips)


def plan(owners):
    half = owners // 2
    far, near = list(range(half, owners)), list(range(1, half))
    flips = woven(far, near)
    due = []
    for c in range(CHUNKS):
        place = half * (c + 1) + FAR
        due.append((min(place, half * (CHUNKS + c)), ("gram", c)))
        due.append((min(place + LATER, half * (CHUNKS + c)), ("apply", c)))
        if c:
            due.append((half * (c - 1) + FAR - 1, ("momentum", c, tuple(flips + [0]))))
        if c < CHUNKS - 1:
            due.append((half * (CHUNKS + c + 1) + FAR, ("weights", c, tuple([0] + flips))))
    due.sort(key=lambda one: one[0])
    steps, gone = [], 0
    heads = cut(flips + [0], HEAD)
    steps.append(("momentum", 0, heads[0]))
    rest, ready = heads[1:], set(heads[0])
    for kind in ("in", "out"):
        for c in range(CHUNKS):
            order = flips if (kind, c) != ("out", CHUNKS - 1) else woven(far[:-TAIL], near) + far[-TAIL:]
            for flip in order:
                while kind == "in" and c == 0 and flip not in ready:
                    steps.append(("momentum", 0, rest[0]))
                    ready |= set(rest.pop(0))
                while flip in far and due and due[0][0] <= gone:
                    steps.append(due.pop(0)[1])
                steps.append((kind, c, flip))
                gone += flip in far
    steps += [one for _, one in due]
    return steps + [("weights", CHUNKS - 1, run) for run in cut([0] + order, LAST)]


def body(gradients, momentum, weights):
    owners = lax.axis_size("shard")
    mats, _, _ = gradients.shape
    held = mats // (CHUNKS * owners)
    tick = lax.axis_index("shard").astype(jnp.int32)
    me = tick.reshape(1)
    whole, updated, ticks = None, None, 0
    pieces, arrived, grams, found, back = {}, {}, {}, {}, {}
    ends, gates = {True: [], False: []}, []

    def send(piece, flip):
        far = flip >= owners // 2
        window = FAR if far else NEAR
        before = gates + ends[far][-window:][:len(ends[far]) >= window]
        if before:
            piece = lax.optimization_barrier((piece, *before))[0]
        gates.clear()
        ends[far].append(lax.ppermute(piece, "shard", [(i, i ^ flip) for i in range(owners)]))
        return ends[far][-1]

    for kind, c, *more in plan(owners):
        if kind == "momentum":
            whole, *some = momentum_of(me, more[0], c, held, gradients, momentum, whole)
            pieces.update(zip([(c, flip) for flip in more[0]], some))
            gates.append(whole)
        elif kind == "in":
            arrived[c, more[0]] = send(pieces[c, more[0]], more[0])
        elif kind == "gram":
            arrived[c, 0] = pieces[c, 0]
            grams[c] = [gram_of([arrived[c, flip] for flip in range(owners)])]
            gates.append(grams[c][0])
        elif kind == "apply":
            outs = apply_of(grams[c], [arrived[c, flip] for flip in range(owners)])
            found.update({(c, flip): out for flip, out in enumerate(outs)})
            back[c, 0] = outs[0]
            gates.append(outs[0])
        elif kind == "out":
            back[c, more[0]] = send(found[c, more[0]], more[0])
        elif kind == "weights":
            updated = weights_of((lax.optimization_barrier(tick) - ticks).reshape(1), more[0], c, weights, [back[c, flip] for flip in more[0]], updated)
            gates.append(updated)
        if kind in ("in", "out"):
            tick, ticks = lax.optimization_barrier(tick) + 1, ticks + 1
        if kind == "gram":
            grams[c] += around(grams[c][0], "model")
    return (updated, whole)


def small_body(gradients, momentum, weights):
    new_momentum = hold_rate * momentum + gradients
    stack = lax.all_to_all(new_momentum, "shard", split_axis=0, concat_axis=1, tiled=True)
    gram = mm("mik,mjk->mij", stack, stack)
    gram = gram + sum(around(gram, "model"))
    chain = polynomial(gram, functools.partial(mm, "mij,mjk->mik"))
    back = lax.all_to_all(mm("mij,mjk->mik", chain, stack), "shard", split_axis=1, concat_axis=0, tiled=True)
    return ((1.0 - learn_rate * decay_rate) * weights - learn_rate * back, new_momentum)


def pick(gradients, momentum, weights):
    owners = lax.axis_size("shard")
    mats, rows, columns = gradients.shape
    fits = rows % 8 == 0 and columns % 128 == 0 and mats % (CHUNKS * owners) == 0 and owners & (owners - 1) == 0 and owners // 2 >= FAR
    return (body if fits else small_body)(gradients, momentum, weights)


def solution(mesh):
    placed = P(None, "shard", "model")
    return jax.shard_map(pick, mesh=mesh, in_specs=(placed,) * 3, out_specs=(placed,) * 2, check_vma=False)
```

```python
import functools

import jax
import jax.numpy as jnp
from jax import lax
from jax.experimental import pallas as pl
from jax.experimental.pallas import tpu as pltpu
from jax.sharding import PartitionSpec as P


ITERS = 3
CHUNKS = 2
FAR = 6
NEAR = 6
LATER = 1
HEAD = (1, 3, 4)
TAIL = 3
LAST = (8, 4, 3)
VMEM = 52 << 20

hold_rate = 0.9
learn_rate = 0.9
decay_rate = 0.1


def mm(form, a, b):
    return jnp.einsum(form, a, b, precision=lax.Precision.HIGHEST)


def dot(a, b, contract_b=0):
    return lax.dot_general(
        a, b, (((1,), (contract_b,)), ((), ())),
        precision=lax.Precision.HIGHEST, preferred_element_type=jnp.float32,
    )


def cost(flops, moved):
    return pl.CostEstimate(flops=flops, bytes_accessed=moved, transcendentals=0)


def around(part, axis):
    size = lax.axis_size(axis)
    return [lax.ppermute(part, axis, [(i, (i + hop) % size) for i in range(size)]) for hop in range(1, size)]


def polynomial(raw, product):
    side = raw.shape[-1]
    place = raw.shape[:-2] + (side, side)
    eye = (lax.broadcasted_iota(jnp.int32, place, raw.ndim - 2) == lax.broadcasted_iota(jnp.int32, place, raw.ndim - 1)).astype(jnp.float32)
    total = jnp.sum(jnp.sum(raw * eye, axis=-1, keepdims=True), axis=-2, keepdims=True)
    scale = lax.rsqrt(total + 1e-06)
    gram = (raw * scale) * scale
    chain = None
    for step in range(ITERS):
        poly = 3.4445 * eye - 4.775 * gram + 2.0315 * product(gram, gram)
        chain = poly if chain is None else product(poly, chain)
        if step < ITERS - 1:
            gram = product(poly, product(gram, poly))
    return chain * scale


def places(flips, held, rows, columns, chunk):
    def spot(i, me):
        flip = flips[0]
        for k in range(1, len(flips)):
            flip = jnp.where(i == k, flips[k], flip)
        return ((me[0] ^ flip) * CHUNKS + chunk, 0, 0)

    return pl.BlockSpec((held, rows, columns), spot)


def momentum_kernel(count, me_ref, gradients_ref, momentum_ref, *refs):
    whole_ref, piece_refs = refs[-count - 1], refs[-count:]
    fresh = hold_rate * momentum_ref[...] + gradients_ref[...]
    whole_ref[...] = fresh
    for k in range(count):
        @pl.when(pl.program_id(0) == k)
        def _():
            piece_refs[k][...] = fresh


def momentum_of(me, flips, chunk, held, gradients, momentum, whole):
    _, rows, columns = gradients.shape
    count = len(flips)
    there = places(flips, held, rows, columns, chunk)
    here = pl.BlockSpec((held, rows, columns), lambda i, me: (0, 0, 0))
    size = count * held * rows * columns
    more = [] if whole is None else [whole]
    return pl.pallas_call(
        functools.partial(momentum_kernel, count),
        grid_spec=pltpu.PrefetchScalarGridSpec(
            num_scalar_prefetch=1,
            grid=(count,),
            in_specs=[there, there] + [pl.BlockSpec(memory_space=pl.ANY)] * len(more),
            out_specs=[there] + [here] * count,
        ),
        out_shape=[jax.ShapeDtypeStruct(gradients.shape, jnp.float32)]
        + [jax.ShapeDtypeStruct((held, rows, columns), jnp.float32)] * count,
        input_output_aliases={3: 0} if more else {},
        cost_estimate=cost(2 * size, 16 * size),
        name="momentum",
    )(me, gradients, momentum, *more)


def weights_kernel(count, me_ref, weights_ref, *refs):
    for k in range(count):
        @pl.when(pl.program_id(0) == k)
        def _():
            refs[-1][...] = (1.0 - learn_rate * decay_rate) * weights_ref[...] - learn_rate * refs[k][...]


def weights_of(me, flips, chunk, weights, back, whole, landed):
    _, rows, columns = weights.shape
    count, held = len(flips), back[0].shape[0]
    there = places(flips, held, rows, columns, chunk)
    here = pl.BlockSpec(memory_space=pltpu.VMEM) if landed else pl.BlockSpec((held, rows, columns), lambda i, me: (0, 0, 0))
    size = count * held * rows * columns
    more = [] if whole is None else [whole]
    return pl.pallas_call(
        functools.partial(weights_kernel, count),
        grid_spec=pltpu.PrefetchScalarGridSpec(
            num_scalar_prefetch=1,
            grid=(count,),
            in_specs=[there] + [here] * count + [pl.BlockSpec(memory_space=pl.ANY)] * len(more),
            out_specs=there,
        ),
        out_shape=jax.ShapeDtypeStruct(weights.shape, jnp.float32),
        input_output_aliases={2 + count: 0} if more else {},
        compiler_params=pltpu.CompilerParams(vmem_limit_bytes=VMEM),
        cost_estimate=cost(3 * size, 12 * size),
        name="weights",
    )(me, weights, *back, *more)


def stacked(refs):
    return jnp.concatenate([ref[0] for ref in refs], axis=0)


def gram_kernel(*refs):
    stack = stacked(refs[:-1])
    refs[-1][0] = dot(stack, stack, 1)


def gram_of(pieces):
    held, rows, columns = pieces[0].shape
    side = len(pieces) * rows
    return pl.pallas_call(
        gram_kernel,
        grid=(held,),
        in_specs=[pl.BlockSpec((1, rows, columns), lambda i: (i, 0, 0))] * len(pieces),
        out_specs=pl.BlockSpec((1, side, side), lambda i: (i, 0, 0)),
        out_shape=jax.ShapeDtypeStruct((held, side, side), jnp.float32),
        cost_estimate=cost(12 * held * side * side * columns, 4 * held * side * columns),
        name="gram",
    )(*pieces)


def apply_kernel(parts, count, *refs):
    raw = refs[0][0]
    for ref in refs[1:parts]:
        raw = raw + ref[0]
    found = dot(polynomial(raw, dot), stacked(refs[parts:parts + count]))
    rows = found.shape[0] // count
    for k in range(count):
        refs[parts + count + k][0] = found[k * rows:(k + 1) * rows]


def apply_of(grams, pieces):
    held, rows, columns = pieces[0].shape
    side = len(pieces) * rows
    square = pl.BlockSpec((1, side, side), lambda i: (i, 0, 0))
    strip = pl.BlockSpec((1, rows, columns), lambda i: (i, 0, 0))
    return pl.pallas_call(
        functools.partial(apply_kernel, len(grams), len(pieces)),
        grid=(held,),
        in_specs=[square] * len(grams) + [strip] * len(pieces),
        out_specs=[strip] * len(pieces),
        out_shape=[jax.ShapeDtypeStruct((held, rows, columns), jnp.float32)] * len(pieces),
        cost_estimate=cost(12 * held * side * side * (columns + 9 * side), 8 * held * side * columns),
        name="apply",
    )(*grams, *pieces)


def woven(far, near):
    flips = []
    for k in range(max(len(far), len(near))):
        flips += far[k:k + 1] + near[k:k + 1]
    return flips


def cut(flips, sizes):
    runs = []
    for size in sizes:
        runs.append(tuple(flips[:size]))
        flips = flips[size:]
    return runs + [tuple(flips)] * bool(flips)


def plan(owners):
    half = owners // 2
    far, near = list(range(half, owners)), list(range(1, half))
    flips = woven(far, near)
    due = []
    for c in range(CHUNKS):
        place = half * (c + 1) + FAR
        due.append((min(place, half * (CHUNKS + c)), ("gram", c)))
        due.append((min(place + LATER, half * (CHUNKS + c)), ("apply", c)))
        if c:
            due.append((half * (c - 1) + FAR - 1, ("momentum", c, tuple(flips + [0]))))
        if c < CHUNKS - 1:
            due.append((half * (CHUNKS + c + 1) + FAR, ("weights", c, tuple([0] + flips))))
    due.sort(key=lambda one: one[0])
    steps, gone = [], 0
    heads = cut(flips + [0], HEAD)
    steps.append(("momentum", 0, heads[0]))
    rest, ready = heads[1:], set(heads[0])
    for kind in ("in", "out"):
        for c in range(CHUNKS):
            order = flips if (kind, c) != ("out", CHUNKS - 1) else woven(far[:-TAIL], near) + far[-TAIL:]
            for flip in order:
                while kind == "in" and c == 0 and flip not in ready:
                    steps.append(("momentum", 0, rest[0]))
                    ready |= set(rest.pop(0))
                while flip in far and due and due[0][0] <= gone:
                    steps.append(due.pop(0)[1])
                steps.append((kind, c, flip))
                gone += flip in far
    steps += [one for _, one in due]
    return steps + [("weights", CHUNKS - 1, run) for run in cut([0] + order, LAST)]


def body(gradients, momentum, weights):
    owners = lax.axis_size("shard")
    mats, _, _ = gradients.shape
    held = mats // (CHUNKS * owners)
    tick = lax.axis_index("shard").astype(jnp.int32)
    me = tick.reshape(1)
    whole, updated, ticks = None, None, 0
    pieces, arrived, grams, found, back = {}, {}, {}, {}, {}
    ends, gates = {True: [], False: []}, []

    def send(piece, flip):
        far = flip >= owners // 2
        window = FAR if far else NEAR
        before = gates + ends[far][-window:][:len(ends[far]) >= window]
        if before:
            piece = lax.optimization_barrier((piece, *before))[0]
        gates.clear()
        ends[far].append(lax.ppermute(piece, "shard", [(i, i ^ flip) for i in range(owners)]))
        return ends[far][-1]

    for kind, c, *more in plan(owners):
        if kind == "momentum":
            whole, *some = momentum_of(me, more[0], c, held, gradients, momentum, whole)
            pieces.update(zip([(c, flip) for flip in more[0]], some))
            gates.append(whole)
        elif kind == "in":
            arrived[c, more[0]] = send(pieces[c, more[0]], more[0])
        elif kind == "gram":
            arrived[c, 0] = pieces[c, 0]
            grams[c] = [gram_of([arrived[c, flip] for flip in range(owners)])]
            gates.append(grams[c][0])
        elif kind == "apply":
            outs = apply_of(grams[c], [arrived[c, flip] for flip in range(owners)])
            found.update({(c, flip): out for flip, out in enumerate(outs)})
            back[c, 0] = outs[0]
            gates.append(outs[0])
        elif kind == "out":
            back[c, more[0]] = send(found[c, more[0]], more[0])
        elif kind == "weights":
            updated = weights_of((lax.optimization_barrier(tick) - ticks).reshape(1), more[0], c, weights, [back[c, flip] for flip in more[0]], updated, len(more[0]) < owners // 2)
            gates.append(updated)
        if kind in ("in", "out"):
            tick, ticks = lax.optimization_barrier(tick) + 1, ticks + 1
        if kind == "gram":
            grams[c] += around(grams[c][0], "model")
    return (updated, whole)


def small_body(gradients, momentum, weights):
    new_momentum = hold_rate * momentum + gradients
    stack = lax.all_to_all(new_momentum, "shard", split_axis=0, concat_axis=1, tiled=True)
    gram = mm("mik,mjk->mij", stack, stack)
    gram = gram + sum(around(gram, "model"))
    chain = polynomial(gram, functools.partial(mm, "mij,mjk->mik"))
    back = lax.all_to_all(mm("mij,mjk->mik", chain, stack), "shard", split_axis=1, concat_axis=0, tiled=True)
    return ((1.0 - learn_rate * decay_rate) * weights - learn_rate * back, new_momentum)


def pick(gradients, momentum, weights):
    owners = lax.axis_size("shard")
    mats, rows, columns = gradients.shape
    fits = rows % 8 == 0 and columns % 128 == 0 and mats % (CHUNKS * owners) == 0 and owners & (owners - 1) == 0 and owners // 2 >= FAR
    return (body if fits else small_body)(gradients, momentum, weights)


def solution(mesh):
    placed = P(None, "shard", "model")
    return jax.shard_map(pick, mesh=mesh, in_specs=(placed,) * 3, out_specs=(placed,) * 2, check_vma=False)
```

```python
import functools

import jax
import jax.numpy as jnp
from jax import lax
from jax.experimental import pallas as pl
from jax.experimental.pallas import tpu as pltpu
from jax.sharding import PartitionSpec as P


ITERS = 3
CHUNKS = 2
FAR = 6
NEAR = 6
LATER = 1
HEAD = (1, 3, 4)
TAIL = 3
LAST = (8, 4)
LEAD = 1
VMEM = 52 << 20

hold_rate = 0.9
learn_rate = 0.9
decay_rate = 0.1


def mm(form, a, b):
    return jnp.einsum(form, a, b, precision=lax.Precision.HIGHEST)


def dot(a, b, contract_b=0):
    return lax.dot_general(
        a, b, (((1,), (contract_b,)), ((), ())),
        precision=lax.Precision.HIGHEST, preferred_element_type=jnp.float32,
    )


def cost(flops, moved):
    return pl.CostEstimate(flops=flops, bytes_accessed=moved, transcendentals=0)


def around(part, axis):
    size = lax.axis_size(axis)
    return [lax.ppermute(part, axis, [(i, (i + hop) % size) for i in range(size)]) for hop in range(1, size)]


def polynomial(raw, product):
    side = raw.shape[-1]
    place = raw.shape[:-2] + (side, side)
    eye = (lax.broadcasted_iota(jnp.int32, place, raw.ndim - 2) == lax.broadcasted_iota(jnp.int32, place, raw.ndim - 1)).astype(jnp.float32)
    total = jnp.sum(jnp.sum(raw * eye, axis=-1, keepdims=True), axis=-2, keepdims=True)
    scale = lax.rsqrt(total + 1e-06)
    gram = (raw * scale) * scale
    chain = None
    for step in range(ITERS):
        poly = 3.4445 * eye - 4.775 * gram + 2.0315 * product(gram, gram)
        chain = poly if chain is None else product(poly, chain)
        if step < ITERS - 1:
            gram = product(poly, product(gram, poly))
    return chain * scale


def places(flips, held, rows, columns, chunk):
    def spot(i, me):
        flip = flips[0]
        for k in range(1, len(flips)):
            flip = jnp.where(i == k, flips[k], flip)
        return ((me[0] ^ flip) * CHUNKS + chunk, 0, 0)

    return pl.BlockSpec((held, rows, columns), spot)


def momentum_kernel(count, me_ref, gradients_ref, momentum_ref, *refs):
    whole_ref, piece_refs = refs[-count - 1], refs[-count:]
    fresh = hold_rate * momentum_ref[...] + gradients_ref[...]
    whole_ref[...] = fresh
    for k in range(count):
        @pl.when(pl.program_id(0) == k)
        def _():
            piece_refs[k][...] = fresh


def momentum_of(me, flips, chunk, held, gradients, momentum, whole):
    _, rows, columns = gradients.shape
    count = len(flips)
    there = places(flips, held, rows, columns, chunk)
    here = pl.BlockSpec((held, rows, columns), lambda i, me: (0, 0, 0))
    size = count * held * rows * columns
    more = [] if whole is None else [whole]
    return pl.pallas_call(
        functools.partial(momentum_kernel, count),
        grid_spec=pltpu.PrefetchScalarGridSpec(
            num_scalar_prefetch=1,
            grid=(count,),
            in_specs=[there, there] + [pl.BlockSpec(memory_space=pl.ANY)] * len(more),
            out_specs=[there] + [here] * count,
        ),
        out_shape=[jax.ShapeDtypeStruct(gradients.shape, jnp.float32)]
        + [jax.ShapeDtypeStruct((held, rows, columns), jnp.float32)] * count,
        input_output_aliases={3: 0} if more else {},
        cost_estimate=cost(2 * size, 16 * size),
        name="momentum",
    )(me, gradients, momentum, *more)


def weights_kernel(count, me_ref, weights_ref, *refs):
    for k in range(count):
        @pl.when(pl.program_id(0) == k)
        def _():
            refs[-1][...] = (1.0 - learn_rate * decay_rate) * weights_ref[...] - learn_rate * refs[k][...]


def weights_of(me, flips, chunk, weights, back, whole, landed):
    _, rows, columns = weights.shape
    count, held = len(flips), back[0].shape[0]
    there = places(flips, held, rows, columns, chunk)
    here = pl.BlockSpec(memory_space=pltpu.VMEM) if landed else pl.BlockSpec((held, rows, columns), lambda i, me: (0, 0, 0))
    size = count * held * rows * columns
    more = [] if whole is None else [whole]
    return pl.pallas_call(
        functools.partial(weights_kernel, count),
        grid_spec=pltpu.PrefetchScalarGridSpec(
            num_scalar_prefetch=1,
            grid=(count,),
            in_specs=[there] + [here] * count + [pl.BlockSpec(memory_space=pl.ANY)] * len(more),
            out_specs=there,
        ),
        out_shape=jax.ShapeDtypeStruct(weights.shape, jnp.float32),
        input_output_aliases={2 + count: 0} if more else {},
        compiler_params=pltpu.CompilerParams(vmem_limit_bytes=VMEM),
        cost_estimate=cost(3 * size, 12 * size),
        name="weights",
    )(me, weights, *back, *more)


def ahead_kernel(me_ref, weights_ref, out_ref):
    out_ref[...] = (1.0 - learn_rate * decay_rate) * weights_ref[...]


def close_kernel(me_ref, ready_ref, back_ref, _, out_ref):
    out_ref[...] = ready_ref[...] - learn_rate * back_ref[...]


def ahead_of(me, flip, chunk, held, weights):
    _, rows, columns = weights.shape
    size = held * rows * columns
    return pl.pallas_call(
        ahead_kernel,
        grid_spec=pltpu.PrefetchScalarGridSpec(
            num_scalar_prefetch=1,
            grid=(1,),
            in_specs=[places((flip,), held, rows, columns, chunk)],
            out_specs=pl.BlockSpec((held, rows, columns), lambda i, me: (0, 0, 0)),
        ),
        out_shape=jax.ShapeDtypeStruct((held, rows, columns), jnp.float32),
        compiler_params=pltpu.CompilerParams(vmem_limit_bytes=VMEM),
        cost_estimate=cost(size, 8 * size),
        name="ahead",
    )(me, weights)


def close_of(me, flip, chunk, ready, back, whole):
    held, rows, columns = back.shape
    size = held * rows * columns
    near = pl.BlockSpec(memory_space=pltpu.VMEM)
    return pl.pallas_call(
        close_kernel,
        grid_spec=pltpu.PrefetchScalarGridSpec(
            num_scalar_prefetch=1,
            grid=(1,),
            in_specs=[near, near, pl.BlockSpec(memory_space=pl.ANY)],
            out_specs=places((flip,), held, rows, columns, chunk),
        ),
        out_shape=jax.ShapeDtypeStruct(whole.shape, jnp.float32),
        input_output_aliases={3: 0},
        compiler_params=pltpu.CompilerParams(vmem_limit_bytes=VMEM),
        cost_estimate=cost(2 * size, 12 * size),
        name="close",
    )(me, ready, back, whole)


def stacked(refs):
    return jnp.concatenate([ref[0] for ref in refs], axis=0)


def gram_kernel(*refs):
    stack = stacked(refs[:-1])
    refs[-1][0] = dot(stack, stack, 1)


def gram_of(pieces):
    held, rows, columns = pieces[0].shape
    side = len(pieces) * rows
    return pl.pallas_call(
        gram_kernel,
        grid=(held,),
        in_specs=[pl.BlockSpec((1, rows, columns), lambda i: (i, 0, 0))] * len(pieces),
        out_specs=pl.BlockSpec((1, side, side), lambda i: (i, 0, 0)),
        out_shape=jax.ShapeDtypeStruct((held, side, side), jnp.float32),
        cost_estimate=cost(12 * held * side * side * columns, 4 * held * side * columns),
        name="gram",
    )(*pieces)


def apply_kernel(parts, count, *refs):
    raw = refs[0][0]
    for ref in refs[1:parts]:
        raw = raw + ref[0]
    found = dot(polynomial(raw, dot), stacked(refs[parts:parts + count]))
    rows = found.shape[0] // count
    for k in range(count):
        refs[parts + count + k][0] = found[k * rows:(k + 1) * rows]


def apply_of(grams, pieces):
    held, rows, columns = pieces[0].shape
    side = len(pieces) * rows
    square = pl.BlockSpec((1, side, side), lambda i: (i, 0, 0))
    strip = pl.BlockSpec((1, rows, columns), lambda i: (i, 0, 0))
    return pl.pallas_call(
        functools.partial(apply_kernel, len(grams), len(pieces)),
        grid=(held,),
        in_specs=[square] * len(grams) + [strip] * len(pieces),
        out_specs=[strip] * len(pieces),
        out_shape=[jax.ShapeDtypeStruct((held, rows, columns), jnp.float32)] * len(pieces),
        cost_estimate=cost(12 * held * side * side * (columns + 9 * side), 8 * held * side * columns),
        name="apply",
    )(*grams, *pieces)


def woven(far, near):
    flips = []
    for k in range(max(len(far), len(near))):
        flips += far[k:k + 1] + near[k:k + 1]
    return flips


def cut(flips, sizes):
    runs = []
    for size in sizes:
        runs.append(tuple(flips[:size]))
        flips = flips[size:]
    return runs + [tuple(flips)] * bool(flips)


def plan(owners):
    half = owners // 2
    far, near = list(range(half, owners)), list(range(1, half))
    flips = woven(far, near)
    due = []
    for c in range(CHUNKS):
        place = half * (c + 1) + FAR
        due.append((min(place, half * (CHUNKS + c)), ("gram", c)))
        due.append((min(place + LATER, half * (CHUNKS + c)), ("apply", c)))
        if c:
            due.append((half * (c - 1) + FAR - 1, ("momentum", c, tuple(flips + [0]))))
        if c < CHUNKS - 1:
            due.append((half * (CHUNKS + c + 1) + FAR, ("weights", c, tuple([0] + flips))))
    due.sort(key=lambda one: one[0])
    steps, gone = [], 0
    first = woven(far[half // 2:half // 2 + LEAD] + far[:half // 2] + far[half // 2 + LEAD:], near)
    heads = cut(first + [0], HEAD)
    steps.append(("momentum", 0, heads[0]))
    rest, ready = heads[1:], set(heads[0])
    for kind in ("in", "out"):
        for c in range(CHUNKS):
            order = flips if (kind, c) != ("out", CHUNKS - 1) else woven(far[:-TAIL], near) + far[-TAIL:]
            order = first if (kind, c) == ("in", 0) else order
            for flip in order:
                while kind == "in" and c == 0 and flip not in ready:
                    steps.append(("momentum", 0, rest[0]))
                    ready |= set(rest.pop(0))
                while flip in far and due and due[0][0] <= gone:
                    steps.append(due.pop(0)[1])
                steps.append((kind, c, flip))
                gone += flip in far
    steps += [one for _, one in due]
    steps.append(("ahead", CHUNKS - 1, order[-1]))
    steps += [("weights", CHUNKS - 1, run) for run in cut([0] + order[:-1], LAST)]
    return steps + [("close", CHUNKS - 1, order[-1])]


def body(gradients, momentum, weights):
    owners = lax.axis_size("shard")
    mats, _, _ = gradients.shape
    held = mats // (CHUNKS * owners)
    tick = lax.axis_index("shard").astype(jnp.int32)
    me = tick.reshape(1)
    whole, updated, ticks = None, None, 0
    pieces, arrived, grams, found, back = {}, {}, {}, {}, {}
    ends, gates = {True: [], False: []}, []

    def send(piece, flip):
        far = flip >= owners // 2
        window = FAR if far else NEAR
        before = gates + ends[far][-window:][:len(ends[far]) >= window]
        if before:
            piece = lax.optimization_barrier((piece, *before))[0]
        gates.clear()
        ends[far].append(lax.ppermute(piece, "shard", [(i, i ^ flip) for i in range(owners)]))
        return ends[far][-1]

    for kind, c, *more in plan(owners):
        if kind == "momentum":
            whole, *some = momentum_of(me, more[0], c, held, gradients, momentum, whole)
            pieces.update(zip([(c, flip) for flip in more[0]], some))
            gates.append(whole)
        elif kind == "in":
            arrived[c, more[0]] = send(pieces[c, more[0]], more[0])
        elif kind == "gram":
            arrived[c, 0] = pieces[c, 0]
            grams[c] = [gram_of([arrived[c, flip] for flip in range(owners)])]
            gates.append(grams[c][0])
        elif kind == "apply":
            outs = apply_of(grams[c], [arrived[c, flip] for flip in range(owners)])
            found.update({(c, flip): out for flip, out in enumerate(outs)})
            back[c, 0] = outs[0]
            gates.append(outs[0])
        elif kind == "out":
            back[c, more[0]] = send(found[c, more[0]], more[0])
        elif kind == "weights":
            updated = weights_of((lax.optimization_barrier(tick) - ticks).reshape(1), more[0], c, weights, [back[c, flip] for flip in more[0]], updated, len(more[0]) < owners // 2)
            gates.append(updated)
        elif kind == "ahead":
            ready = ahead_of(me, more[0], c, held, weights)
        elif kind == "close":
            updated = close_of(me, more[0], c, ready, back[c, more[0]], updated)
        if kind in ("in", "out"):
            tick, ticks = lax.optimization_barrier(tick) + 1, ticks + 1
        if kind == "gram":
            grams[c] += around(grams[c][0], "model")
    return (updated, whole)


def small_body(gradients, momentum, weights):
    new_momentum = hold_rate * momentum + gradients
    stack = lax.all_to_all(new_momentum, "shard", split_axis=0, concat_axis=1, tiled=True)
    gram = mm("mik,mjk->mij", stack, stack)
    gram = gram + sum(around(gram, "model"))
    chain = polynomial(gram, functools.partial(mm, "mij,mjk->mik"))
    back = lax.all_to_all(mm("mij,mjk->mik", chain, stack), "shard", split_axis=1, concat_axis=0, tiled=True)
    return ((1.0 - learn_rate * decay_rate) * weights - learn_rate * back, new_momentum)


def pick(gradients, momentum, weights):
    owners = lax.axis_size("shard")
    mats, rows, columns = gradients.shape
    fits = rows % 8 == 0 and columns % 128 == 0 and mats % (CHUNKS * owners) == 0 and owners & (owners - 1) == 0 and owners // 2 >= FAR
    return (body if fits else small_body)(gradients, momentum, weights)


def solution(mesh):
    placed = P(None, "shard", "model")
    return jax.shard_map(pick, mesh=mesh, in_specs=(placed,) * 3, out_specs=(placed,) * 2, check_vma=False)
```

```python
import functools

import jax
import jax.numpy as jnp
from jax import lax
from jax.experimental import pallas as pl
from jax.experimental.pallas import tpu as pltpu
from jax.sharding import PartitionSpec as P


ITERS = 3
CHUNKS = 2
FAR = 6
NEAR = 7
LATER = 1
HEAD = (1, 3, 4)
TAIL = 3
LAST = (8, 4)
LEAD = 1
VMEM = 52 << 20

hold_rate = 0.9
learn_rate = 0.9
decay_rate = 0.1


def mm(form, a, b):
    return jnp.einsum(form, a, b, precision=lax.Precision.HIGHEST)


def dot(a, b, contract_b=0):
    return lax.dot_general(
        a, b, (((1,), (contract_b,)), ((), ())),
        precision=lax.Precision.HIGHEST, preferred_element_type=jnp.float32,
    )


def cost(flops, moved):
    return pl.CostEstimate(flops=flops, bytes_accessed=moved, transcendentals=0)


def around(part, axis):
    size = lax.axis_size(axis)
    return [lax.ppermute(part, axis, [(i, (i + hop) % size) for i in range(size)]) for hop in range(1, size)]


def polynomial(raw, product):
    side = raw.shape[-1]
    place = raw.shape[:-2] + (side, side)
    eye = (lax.broadcasted_iota(jnp.int32, place, raw.ndim - 2) == lax.broadcasted_iota(jnp.int32, place, raw.ndim - 1)).astype(jnp.float32)
    total = jnp.sum(jnp.sum(raw * eye, axis=-1, keepdims=True), axis=-2, keepdims=True)
    scale = lax.rsqrt(total + 1e-06)
    gram = (raw * scale) * scale
    chain = None
    for step in range(ITERS):
        poly = 3.4445 * eye - 4.775 * gram + 2.0315 * product(gram, gram)
        chain = poly if chain is None else product(poly, chain)
        if step < ITERS - 1:
            gram = product(poly, product(gram, poly))
    return chain * scale


def places(flips, held, rows, columns, chunk):
    def spot(i, me):
        flip = flips[0]
        for k in range(1, len(flips)):
            flip = jnp.where(i == k, flips[k], flip)
        return ((me[0] ^ flip) * CHUNKS + chunk, 0, 0)

    return pl.BlockSpec((held, rows, columns), spot)


def momentum_kernel(count, me_ref, gradients_ref, momentum_ref, *refs):
    whole_ref, piece_refs = refs[-count - 1], refs[-count:]
    fresh = hold_rate * momentum_ref[...] + gradients_ref[...]
    whole_ref[...] = fresh
    for k in range(count):
        @pl.when(pl.program_id(0) == k)
        def _():
            piece_refs[k][...] = fresh


def momentum_of(me, flips, chunk, held, gradients, momentum, whole):
    _, rows, columns = gradients.shape
    count = len(flips)
    there = places(flips, held, rows, columns, chunk)
    here = pl.BlockSpec((held, rows, columns), lambda i, me: (0, 0, 0))
    size = count * held * rows * columns
    more = [] if whole is None else [whole]
    return pl.pallas_call(
        functools.partial(momentum_kernel, count),
        grid_spec=pltpu.PrefetchScalarGridSpec(
            num_scalar_prefetch=1,
            grid=(count,),
            in_specs=[there, there] + [pl.BlockSpec(memory_space=pl.ANY)] * len(more),
            out_specs=[there] + [here] * count,
        ),
        out_shape=[jax.ShapeDtypeStruct(gradients.shape, jnp.float32)]
        + [jax.ShapeDtypeStruct((held, rows, columns), jnp.float32)] * count,
        input_output_aliases={3: 0} if more else {},
        cost_estimate=cost(2 * size, 16 * size),
        name="momentum",
    )(me, gradients, momentum, *more)


def weights_kernel(count, me_ref, weights_ref, *refs):
    for k in range(count):
        @pl.when(pl.program_id(0) == k)
        def _():
            refs[-1][...] = (1.0 - learn_rate * decay_rate) * weights_ref[...] - learn_rate * refs[k][...]


def weights_of(me, flips, chunk, weights, back, whole, landed):
    _, rows, columns = weights.shape
    count, held = len(flips), back[0].shape[0]
    there = places(flips, held, rows, columns, chunk)
    here = pl.BlockSpec(memory_space=pltpu.VMEM) if landed else pl.BlockSpec((held, rows, columns), lambda i, me: (0, 0, 0))
    size = count * held * rows * columns
    more = [] if whole is None else [whole]
    return pl.pallas_call(
        functools.partial(weights_kernel, count),
        grid_spec=pltpu.PrefetchScalarGridSpec(
            num_scalar_prefetch=1,
            grid=(count,),
            in_specs=[there] + [here] * count + [pl.BlockSpec(memory_space=pl.ANY)] * len(more),
            out_specs=there,
        ),
        out_shape=jax.ShapeDtypeStruct(weights.shape, jnp.float32),
        input_output_aliases={2 + count: 0} if more else {},
        compiler_params=pltpu.CompilerParams(vmem_limit_bytes=VMEM),
        cost_estimate=cost(3 * size, 12 * size),
        name="weights",
    )(me, weights, *back, *more)


def ahead_kernel(me_ref, weights_ref, out_ref):
    out_ref[...] = (1.0 - learn_rate * decay_rate) * weights_ref[...]


def close_kernel(me_ref, ready_ref, back_ref, _, out_ref):
    out_ref[...] = ready_ref[...] - learn_rate * back_ref[...]


def ahead_of(me, flip, chunk, held, weights):
    _, rows, columns = weights.shape
    size = held * rows * columns
    return pl.pallas_call(
        ahead_kernel,
        grid_spec=pltpu.PrefetchScalarGridSpec(
            num_scalar_prefetch=1,
            grid=(1,),
            in_specs=[places((flip,), held, rows, columns, chunk)],
            out_specs=pl.BlockSpec((held, rows, columns), lambda i, me: (0, 0, 0)),
        ),
        out_shape=jax.ShapeDtypeStruct((held, rows, columns), jnp.float32),
        compiler_params=pltpu.CompilerParams(vmem_limit_bytes=VMEM),
        cost_estimate=cost(size, 8 * size),
        name="ahead",
    )(me, weights)


def close_of(me, flip, chunk, ready, back, whole):
    held, rows, columns = back.shape
    size = held * rows * columns
    near = pl.BlockSpec(memory_space=pltpu.VMEM)
    return pl.pallas_call(
        close_kernel,
        grid_spec=pltpu.PrefetchScalarGridSpec(
            num_scalar_prefetch=1,
            grid=(1,),
            in_specs=[near, near, pl.BlockSpec(memory_space=pl.ANY)],
            out_specs=places((flip,), held, rows, columns, chunk),
        ),
        out_shape=jax.ShapeDtypeStruct(whole.shape, jnp.float32),
        input_output_aliases={3: 0},
        compiler_params=pltpu.CompilerParams(vmem_limit_bytes=VMEM),
        cost_estimate=cost(2 * size, 12 * size),
        name="close",
    )(me, ready, back, whole)


def stacked(refs):
    return jnp.concatenate([ref[0] for ref in refs], axis=0)


def gram_kernel(*refs):
    stack = stacked(refs[:-1])
    refs[-1][0] = dot(stack, stack, 1)


def gram_of(pieces):
    held, rows, columns = pieces[0].shape
    side = len(pieces) * rows
    return pl.pallas_call(
        gram_kernel,
        grid=(held,),
        in_specs=[pl.BlockSpec((1, rows, columns), lambda i: (i, 0, 0))] * len(pieces),
        out_specs=pl.BlockSpec((1, side, side), lambda i: (i, 0, 0)),
        out_shape=jax.ShapeDtypeStruct((held, side, side), jnp.float32),
        cost_estimate=cost(12 * held * side * side * columns, 4 * held * side * columns),
        name="gram",
    )(*pieces)


def apply_kernel(parts, count, *refs):
    raw = refs[0][0]
    for ref in refs[1:parts]:
        raw = raw + ref[0]
    found = dot(polynomial(raw, dot), stacked(refs[parts:parts + count]))
    rows = found.shape[0] // count
    for k in range(count):
        refs[parts + count + k][0] = found[k * rows:(k + 1) * rows]


def apply_of(grams, pieces):
    held, rows, columns = pieces[0].shape
    side = len(pieces) * rows
    square = pl.BlockSpec((1, side, side), lambda i: (i, 0, 0))
    strip = pl.BlockSpec((1, rows, columns), lambda i: (i, 0, 0))
    return pl.pallas_call(
        functools.partial(apply_kernel, len(grams), len(pieces)),
        grid=(held,),
        in_specs=[square] * len(grams) + [strip] * len(pieces),
        out_specs=[strip] * len(pieces),
        out_shape=[jax.ShapeDtypeStruct((held, rows, columns), jnp.float32)] * len(pieces),
        cost_estimate=cost(12 * held * side * side * (columns + 9 * side), 8 * held * side * columns),
        name="apply",
    )(*grams, *pieces)


def woven(far, near):
    flips = []
    for k in range(max(len(far), len(near))):
        flips += far[k:k + 1] + near[k:k + 1]
    return flips


def cut(flips, sizes):
    runs = []
    for size in sizes:
        runs.append(tuple(flips[:size]))
        flips = flips[size:]
    return runs + [tuple(flips)] * bool(flips)


def plan(owners):
    half = owners // 2
    far, near = list(range(half, owners)), list(range(1, half))
    flips = woven(far, near)
    due = []
    for c in range(CHUNKS):
        place = half * (c + 1) + FAR
        due.append((min(place, half * (CHUNKS + c)), ("gram", c)))
        due.append((min(place + LATER, half * (CHUNKS + c)), ("apply", c)))
        if c:
            due.append((half * (c - 1) + FAR - 1, ("momentum", c, tuple(flips + [0]))))
        if c < CHUNKS - 1:
            due.append((half * (CHUNKS + c + 1) + FAR, ("weights", c, tuple([0] + flips))))
    due.sort(key=lambda one: one[0])
    steps, gone = [], 0
    lasts = [flip for flip in far if flip != far[half // 2]] + [far[half // 2]]
    first = woven(far[half // 2:half // 2 + LEAD] + far[:half // 2] + far[half // 2 + LEAD:], near)
    heads = cut(first + [0], HEAD)
    steps.append(("momentum", 0, heads[0]))
    rest, ready = heads[1:], set(heads[0])
    for kind in ("in", "out"):
        for c in range(CHUNKS):
            order = flips if (kind, c) != ("out", CHUNKS - 1) else woven(lasts[:-TAIL], near) + lasts[-TAIL:]
            order = first if (kind, c) == ("in", 0) else order
            for flip in order:
                while kind == "in" and c == 0 and flip not in ready:
                    steps.append(("momentum", 0, rest[0]))
                    ready |= set(rest.pop(0))
                while flip in far and due and due[0][0] <= gone:
                    steps.append(due.pop(0)[1])
                steps.append((kind, c, flip))
                gone += flip in far
    steps += [one for _, one in due]
    steps.append(("ahead", CHUNKS - 1, order[-1]))
    steps += [("weights", CHUNKS - 1, run) for run in cut([0] + order[:-1], LAST)]
    return steps + [("close", CHUNKS - 1, order[-1])]


def body(gradients, momentum, weights):
    owners = lax.axis_size("shard")
    mats, _, _ = gradients.shape
    held = mats // (CHUNKS * owners)
    tick = lax.axis_index("shard").astype(jnp.int32)
    me = tick.reshape(1)
    whole, updated, ticks = None, None, 0
    pieces, arrived, grams, found, back = {}, {}, {}, {}, {}
    ends, gates = {True: [], False: []}, []

    def send(piece, flip):
        far = flip >= owners // 2
        window = FAR if far else NEAR
        before = gates + ends[far][-window:][:len(ends[far]) >= window]
        if before:
            piece = lax.optimization_barrier((piece, *before))[0]
        gates.clear()
        ends[far].append(lax.ppermute(piece, "shard", [(i, i ^ flip) for i in range(owners)]))
        return ends[far][-1]

    for kind, c, *more in plan(owners):
        if kind == "momentum":
            whole, *some = momentum_of(me, more[0], c, held, gradients, momentum, whole)
            pieces.update(zip([(c, flip) for flip in more[0]], some))
            gates.append(whole)
        elif kind == "in":
            arrived[c, more[0]] = send(pieces[c, more[0]], more[0])
        elif kind == "gram":
            arrived[c, 0] = pieces[c, 0]
            grams[c] = [gram_of([arrived[c, flip] for flip in range(owners)])]
            gates.append(grams[c][0])
        elif kind == "apply":
            outs = apply_of(grams[c], [arrived[c, flip] for flip in range(owners)])
            found.update({(c, flip): out for flip, out in enumerate(outs)})
            back[c, 0] = outs[0]
            gates.append(outs[0])
        elif kind == "out":
            back[c, more[0]] = send(found[c, more[0]], more[0])
        elif kind == "weights":
            updated = weights_of((lax.optimization_barrier(tick) - ticks).reshape(1), more[0], c, weights, [back[c, flip] for flip in more[0]], updated, len(more[0]) < owners // 2)
            gates.append(updated)
        elif kind == "ahead":
            ready = ahead_of(me, more[0], c, held, weights)
        elif kind == "close":
            updated = close_of(me, more[0], c, ready, back[c, more[0]], updated)
        if kind in ("in", "out"):
            tick, ticks = lax.optimization_barrier(tick) + 1, ticks + 1
        if kind == "gram":
            grams[c] += around(grams[c][0], "model")
    return (updated, whole)


def small_body(gradients, momentum, weights):
    new_momentum = hold_rate * momentum + gradients
    stack = lax.all_to_all(new_momentum, "shard", split_axis=0, concat_axis=1, tiled=True)
    gram = mm("mik,mjk->mij", stack, stack)
    gram = gram + sum(around(gram, "model"))
    chain = polynomial(gram, functools.partial(mm, "mij,mjk->mik"))
    back = lax.all_to_all(mm("mij,mjk->mik", chain, stack), "shard", split_axis=1, concat_axis=0, tiled=True)
    return ((1.0 - learn_rate * decay_rate) * weights - learn_rate * back, new_momentum)


def pick(gradients, momentum, weights):
    owners = lax.axis_size("shard")
    mats, rows, columns = gradients.shape
    fits = rows % 8 == 0 and columns % 128 == 0 and mats % (CHUNKS * owners) == 0 and owners & (owners - 1) == 0 and owners // 2 >= FAR
    return (body if fits else small_body)(gradients, momentum, weights)


def solution(mesh):
    placed = P(None, "shard", "model")
    return jax.shard_map(pick, mesh=mesh, in_specs=(placed,) * 3, out_specs=(placed,) * 2, check_vma=False)
```
